32 devices in a mesh: group: 2 (over y), expert: 8 (over z, x), tensor: 2 (over core).
Axes of the slice: x: 2, y: 2, z: 4, core: 2. Of those that a mesh axis runs over, the one named last changes fastest.
Arguments:
- tokens: bfloat16 [16, 256, 1280], P(('group', 'expert'), 'tensor'), parts along dimension 0, may hold values from -6 to 6
- ln_gain: float32 [1280], replicated, may hold values from 0.5 to 1.5
- slot_keys: bfloat16 [1280, 8], P(None, 'expert'), may hold values from -0.3125 to 0.3125
- w_gate: bfloat16 [8, 1280, 1280], P('expert', 'tensor'), may hold values from -0.15625 to 0.15625
- w_up: bfloat16 [8, 1280, 1280], P('expert', 'tensor'), may hold values from -0.15625 to 0.15625
- w_down: bfloat16 [8, 1280, 1280], P('expert', 'tensor'), may hold values from -0.25 to 0.25
Outputs:
- output: bfloat16 [16, 256, 1280], P(('group', 'expert'), 'tensor'), parts along dimension 0
The draws below stay inside these ranges and needn't reach their ends.
There are 2 independent parts, one for each index of `group`. The reference program is written for one: setup_inputs(seed, part) draws one part's arguments, and reference() takes and returns one part's arrays. A program takes and returns all parts, laid end to end along the dimension named above; an argument that names none is the same for every part. Nothing has to cross between parts.
All inputs are finite; a program needn't handle non-finite values.
Results may differ from the reference program's by a relative error of at most 0.0034.
Values may be sent and summed in bfloat16 or wider, within the bound.
No kernel may reach another device: no remote copies, remote signals or barrier semaphores. Data moves between devices by JAX's collectives and lax.ppermute only.
A program may use at most 64 MiB of HBM per device.

```python
import jax
import jax.numpy as jnp
from jax import lax

D = 1280
FF = 2560
PATCHES = 256
PER_EXPERT = 2
SLOTS = 8
EXPERTS = 4
IMAGES = 8


def block_scale(rng, extent, cuts, least, high):
    level, own = 1.0, jax.random.fold_in(rng, 6)
    for dim, parts in cuts:
        steps = jnp.exp(jax.random.uniform(jax.random.fold_in(own, dim), (parts,), jnp.float32, least / len(cuts), high / len(cuts)))
        level = level * jnp.repeat(steps, extent[dim] // parts).reshape([-1 if axis == dim else 1 for axis in range(len(extent))])
    return level


def centred(rng, extent, scale, most, cuts=(), held_as=jnp.bfloat16):
    array = jax.random.normal(rng, extent, jnp.float32) * scale
    if len(cuts) > 0:
        array = block_scale(rng, extent, cuts, -0.22, 0.18) * array
    return jnp.clip(array, min=-most, max=most).astype(held_as)


def setup_inputs(seed: int = 0, part: int = 0) -> dict:
    key_of = jax.random.split(jax.random.key(seed), 7)
    own_keys = jax.random.split(jax.random.fold_in(key_of[6], part), 7)
    return {
        "tokens": centred(own_keys[0], (IMAGES, PATCHES, D), 1.0, 6.0, ((0, 8), (1, 2))),
        "ln_gain": jnp.clip(1.0 + 0.1 * jax.random.normal(key_of[1], (D,), jnp.float32), 0.5, 1.5),
        "slot_keys": centred(key_of[2], (D, SLOTS), (D // 4) ** -0.5, 0.3125, ((1, 8),)),
        "w_gate": centred(key_of[3], (2 * EXPERTS, FF // 2, D), D ** -0.5, 0.15625, ((0, 8), (1, 2))),
        "w_up": centred(key_of[4], (2 * EXPERTS, FF // 2, D), D ** -0.5, 0.15625, ((0, 8), (1, 2))),
        "w_down": centred(key_of[5], (2 * EXPERTS, FF // 2, D), (FF // 4) ** -0.5, 0.25, ((0, 8), (1, 2))),
    }


epsilon = 1e-06
soft_cap = 20.0

def layer_norm(tokens, ln_gain):
    widened = tokens.astype(jnp.float32)
    center = widened - lax.optimization_barrier(jnp.mean(widened, axis=-1, keepdims=True))
    variance = lax.optimization_barrier(jnp.mean(center * center, axis=-1, keepdims=True))
    return (center * lax.rsqrt(variance + epsilon) * ln_gain.astype(jnp.float32)).astype(jnp.bfloat16)

def apply_expert(operands):
    rows, gate_w, up_w, down_w = operands
    gate_act = jnp.dot(rows, gate_w.T, preferred_element_type=jnp.float32)
    up_proj = jnp.dot(rows, up_w.T, preferred_element_type=jnp.float32)
    hidden = (jax.nn.silu(gate_act) * up_proj).astype(jnp.bfloat16)
    return jnp.dot(hidden, down_w, preferred_element_type=jnp.float32).astype(jnp.bfloat16)

def reference(tokens, ln_gain, slot_keys, w_gate, w_up, w_down):
    normed = layer_norm(tokens, ln_gain)
    raw_scores = jnp.dot(normed.reshape(-1, D), slot_keys, preferred_element_type=jnp.float32)
    raw_scores = raw_scores.reshape(IMAGES, PATCHES, SLOTS)
    scores = jnp.exp(soft_cap * jnp.tanh(raw_scores / soft_cap))
    scores16 = scores.astype(jnp.bfloat16)
    slot_num = jnp.einsum('ips,ipd->isd', scores16.astype(jnp.float32), normed.astype(jnp.float32))
    column_total = lax.optimization_barrier(jnp.sum(scores, axis=1))
    slot_in = (slot_num / column_total[:, :, None]).astype(jnp.bfloat16)
    by_expert = slot_in.reshape(IMAGES, EXPERTS, PER_EXPERT, D).transpose(1, 2, 0, 3)
    by_expert = by_expert.reshape(EXPERTS, PER_EXPERT * IMAGES, D)
    gate_all = w_gate.reshape(EXPERTS, FF, D)
    up_all = w_up.reshape(EXPERTS, FF, D)
    down_all = w_down.reshape(EXPERTS, FF, D)
    slot_out = lax.map(apply_expert, (by_expert, gate_all, up_all, down_all))
    slot_out = slot_out.reshape(EXPERTS, PER_EXPERT, IMAGES, D).transpose(2, 0, 1, 3).reshape(IMAGES, SLOTS, D)
    combine = (scores / lax.optimization_barrier(jnp.sum(scores, axis=2, keepdims=True))).astype(jnp.bfloat16)
    mixed_rows = jnp.einsum('ips,isd->ipd', combine.astype(jnp.float32), slot_out.astype(jnp.float32))
    return (tokens.astype(jnp.float32) + mixed_rows).astype(jnp.bfloat16)
```

```python
import jax
import jax.numpy as jnp
from jax import lax
from jax.sharding import PartitionSpec as P

epsilon = 1e-06
soft_cap = 20.0
per_expert = 2
halves = 2
lanes = 128
everyone = ("expert", "tensor")


def layer_norm(tokens, ln_gain):
    widened = tokens.astype(jnp.float32)
    center = widened - jnp.mean(widened, axis=-1, keepdims=True)
    variance = jnp.mean(center * center, axis=-1, keepdims=True)
    return (center * lax.rsqrt(variance + epsilon) * ln_gain).astype(jnp.bfloat16)


def gather_keys(slot_keys):
    devices = lax.axis_size("expert")
    own = slot_keys.T[None]
    copies = jnp.broadcast_to(own, (devices,) + own.shape[1:])
    arrived = lax.all_to_all(copies, "expert", split_axis=0, concat_axis=0, tiled=True)
    return arrived.reshape(-1, slot_keys.shape[0])


def on_device(tokens, ln_gain, slot_keys, w_gate, w_up, w_down):
    tensor_count = lax.axis_size("tensor")
    devices = lax.axis_size("expert")
    img_dev, half_patches, width = tokens.shape
    all_keys = gather_keys(slot_keys)
    slot_count = all_keys.shape[0]
    experts = slot_count // per_expert
    normed = layer_norm(tokens, ln_gain)
    raw_scores = jnp.einsum("ipd,sd->ips", normed, all_keys, preferred_element_type=jnp.float32)
    scores = jnp.exp(soft_cap * jnp.tanh(raw_scores / soft_cap))
    slot_num = jnp.einsum(
        "ips,ipd->isd", scores.astype(jnp.bfloat16), normed, preferred_element_type=jnp.float32
    )
    column_total = jnp.sum(scores, axis=1)
    combine = (scores / jnp.sum(scores, axis=2, keepdims=True)).astype(jnp.bfloat16)

    coarse = column_total.astype(jnp.bfloat16)
    fine = (column_total - coarse.astype(jnp.float32)).astype(jnp.bfloat16)
    totals = jnp.broadcast_to(coarse[:, :, None], (img_dev, slot_count, lanes // 2))
    rests = jnp.broadcast_to(fine[:, :, None], (img_dev, slot_count, lanes // 2))
    message = jnp.concatenate([slot_num.astype(jnp.bfloat16), totals, rests], axis=2)
    message = message.reshape(img_dev, experts, per_expert, width + lanes)
    message = jnp.transpose(message, (1, 0, 2, 3))[:, None]
    copies = devices * tensor_count // experts
    message = jnp.broadcast_to(message, (experts, copies) + message.shape[2:])
    message = message.reshape(devices * tensor_count, img_dev * per_expert, width + lanes)
    arrived = lax.all_to_all(message, everyone, split_axis=0, concat_axis=0, tiled=True)
    arrived = arrived.reshape(devices, tensor_count, img_dev * per_expert, width + lanes)
    summed = jnp.sum(arrived.astype(jnp.float32), axis=1).reshape(-1, width + lanes)
    total = summed[:, width : width + 1] + summed[:, width + lanes // 2 : width + lanes // 2 + 1]
    rows = (summed[:, :width] / total).astype(jnp.bfloat16)

    contract = (((1,), (1,)), ((), ()))
    gate_act = lax.dot_general(rows, w_gate[0], contract, preferred_element_type=jnp.float32)
    up_proj = lax.dot_general(rows, w_up[0], contract, preferred_element_type=jnp.float32)
    hidden = (jax.nn.silu(gate_act) * up_proj).astype(jnp.bfloat16)
    part_out = jnp.dot(hidden, w_down[0], preferred_element_type=jnp.float32).astype(jnp.bfloat16)

    outgoing = part_out.reshape(devices, 1, img_dev * per_expert, width)
    outgoing = jnp.broadcast_to(outgoing, (devices, tensor_count) + outgoing.shape[2:])
    outgoing = outgoing.reshape(devices * tensor_count, img_dev * per_expert, width)
    returned = lax.all_to_all(outgoing, everyone, split_axis=0, concat_axis=0, tiled=True)
    returned = returned.reshape(experts, copies, img_dev, per_expert, width)
    slot_back = jnp.sum(returned.astype(jnp.float32), axis=1).astype(jnp.bfloat16)
    slot_back = jnp.transpose(slot_back, (1, 0, 2, 3)).reshape(img_dev, slot_count, width)
    mixed_rows = jnp.einsum("ips,isd->ipd", combine, slot_back, preferred_element_type=jnp.float32)
    return (tokens.astype(jnp.float32) + mixed_rows).astype(jnp.bfloat16)


def solution(mesh):
    placed = (
        P(("group", "expert"), "tensor", None),
        P(),
        P(None, "expert"),
        P("expert", "tensor", None),
        P("expert", "tensor", None),
        P("expert", "tensor", None),
    )
    return jax.shard_map(
        on_device,
        mesh=mesh,
        in_specs=placed,
        out_specs=P(("group", "expert"), "tensor", None),
        check_vma=False,
    )
```
